32 devices in a mesh: dp: 8 (over y, x, core), seq: 4 (over z).
Axes of the slice: x: 2, y: 2, z: 4, core: 2. Of those that a mesh axis runs over, the one named last changes fastest.
Arguments:
- block_input: bfloat16 [16, 1032, 1152], P('dp', 'seq'), may hold values from -6 to 6
- skip_input: bfloat16 [16, 1032, 1152], P('dp', None, 'seq'), may hold values from -6 to 6
- key_keep: int32 [16, 1032], P('dp'), may hold values from 0 to 1, as said below
- output_grad: bfloat16 [16, 1032, 1152], P('dp', 'seq'), may hold values from -6 to 6
- skip_weight: float32 [2304, 1152], P('seq', 'dp'), may hold values from -0.125 to 0.125
- skip_first: float32 [2304, 1152], P('seq', 'dp'), may hold values from -192 to 192
- skip_second: float32 [2304, 1152], P('seq', 'dp'), may hold values from 4590.336 to 18377.855
- attend_weight: float32 [1152, 3456], P('seq', 'dp'), may hold values from -0.1875 to 0.1875
- attend_first: float32 [1152, 3456], P('seq', 'dp'), may hold values from -96 to 96
- attend_second: float32 [1152, 3456], P('seq', 'dp'), may hold values from 1149.2352 to 4590.336
- output_weight: float32 [1152, 1152], P('seq', 'dp'), may hold values from -3.5 to 3.5
- output_first: float32 [1152, 1152], P('seq', 'dp'), may hold values from -6 to 6
- output_second: float32 [1152, 1152], P('seq', 'dp'), may hold values from 3.104 to 12.416
- expand_weight: float32 [1152, 4608], P('seq', 'dp'), may hold values from -0.1875 to 0.1875
- expand_first: float32 [1152, 4608], P('seq', 'dp'), may hold values from -40 to 40
- expand_second: float32 [1152, 4608], P('seq', 'dp'), may hold values from 175.8528 to 703.4112
- reduce_weight: float32 [4608, 1152], P('seq', 'dp'), may hold values from -0.125 to 0.125
- reduce_first: float32 [4608, 1152], P('seq', 'dp'), may hold values from -56 to 56
- reduce_second: float32 [4608, 1152], P('seq', 'dp'), may hold values from 366.5664 to 1467.9167
- early_weight: float32 [2, 1152], P(None, 'dp'), may hold values from -0.75 to 0.75
- early_first: float32 [2, 1152], P(None, 'dp'), may hold values from -2048 to 2048
- early_second: float32 [2, 1152], P(None, 'dp'), may hold values from 480618.1 to 1921204.2
- later_weight: float32 [5, 1152], P(None, 'dp'), may hold values from -0.3 to 1.9
- later_first: float32 [5, 1152], P(None, 'dp'), may hold values from -128 to 128
- later_second: float32 [5, 1152], P(None, 'dp'), may hold values from 1948.416 to 7810.176
- hidden_weight: float32 [1, 4608], P(None, 'dp'), may hold values from -6 to 6
- hidden_first: float32 [1, 4608], P(None, 'dp'), may hold values from -40 to 40
- hidden_second: float32 [1, 4608], P(None, 'dp'), may hold values from 175.8528 to 703.4112
Outputs:
- block_output: bfloat16 [16, 1032, 1152], P('dp', 'seq')
- input_grad: bfloat16 [16, 1032, 1152], P('dp', 'seq')
- skip_grad: bfloat16 [16, 1032, 1152], P('dp', None, 'seq')
- skip_master: float32 [2304, 1152], P('seq', 'dp')
- skip_moment: float32 [2304, 1152], P('seq', 'dp')
- skip_square: float32 [2304, 1152], P('seq', 'dp')
- skip_copy: bfloat16 [2304, 1152], P('seq', 'dp')
- attend_master: float32 [1152, 3456], P('seq', 'dp')
- attend_moment: float32 [1152, 3456], P('seq', 'dp')
- attend_square: float32 [1152, 3456], P('seq', 'dp')
- attend_copy: bfloat16 [1152, 3456], P('seq', 'dp')
- output_master: float32 [1152, 1152], P('seq', 'dp')
- output_moment: float32 [1152, 1152], P('seq', 'dp')
- output_square: float32 [1152, 1152], P('seq', 'dp')
- output_copy: bfloat16 [1152, 1152], P('seq', 'dp')
- expand_master: float32 [1152, 4608], P('seq', 'dp')
- expand_moment: float32 [1152, 4608], P('seq', 'dp')
- expand_square: float32 [1152, 4608], P('seq', 'dp')
- expand_copy: bfloat16 [1152, 4608], P('seq', 'dp')
- reduce_master: float32 [4608, 1152], P('seq', 'dp')
- reduce_moment: float32 [4608, 1152], P('seq', 'dp')
- reduce_square: float32 [4608, 1152], P('seq', 'dp')
- reduce_copy: bfloat16 [4608, 1152], P('seq', 'dp')
- early_master: float32 [2, 1152], P(None, 'dp')
- early_moment: float32 [2, 1152], P(None, 'dp')
- early_square: float32 [2, 1152], P(None, 'dp')
- early_copy: bfloat16 [2, 1152], P(None, 'dp')
- later_master: float32 [5, 1152], P(None, 'dp')
- later_moment: float32 [5, 1152], P(None, 'dp')
- later_square: float32 [5, 1152], P(None, 'dp')
- later_copy: bfloat16 [5, 1152], P(None, 'dp')
- hidden_master: float32 [1, 4608], P(None, 'dp')
- hidden_moment: float32 [1, 4608], P(None, 'dp')
- hidden_square: float32 [1, 4608], P(None, 'dp')
- hidden_copy: bfloat16 [1, 4608], P(None, 'dp')
The draws below stay inside these ranges and needn't reach their ends.
Inputs may be any that keep to these rules, and one draw needn't show every extreme that they name: `key_keep`: every image has exactly 6 keys with value 0; all others are 1.
All inputs are finite; a program needn't handle non-finite values.
Results may differ from the reference program's by a relative error of at most 0.023.
Values may be sent and summed in bfloat16 or wider, within the bound.
A program may use at most 320 MiB of HBM per device.

```python
import math
import jax
import jax.numpy as jnp
from jax import lax

D = 1152
H = 16
HD = 72
FF = 4608
L = 1032
PAD = 6
IMAGES = 16
TOKENS_ALL = 16512


def draw_key_keep(key, part):
    row_keys = jax.random.split(key, IMAGES)

    def one_row(row_key):
        shuffled = jax.random.permutation(row_key, L)
        return jnp.where(shuffled < PAD, 0, 1).astype(jnp.int32)
    return jax.vmap(one_row)(row_keys)


def draw_later_weight(key, part):
    gain_key = jax.random.fold_in(key, 11)
    shift_key = jax.random.fold_in(key, 23)
    gains = 1.0 + 0.18 * jnp.clip(jax.random.normal(gain_key, (2, D), jnp.float32), -5.0, 5.0)
    shifts = 0.05 * jnp.clip(jax.random.normal(shift_key, (3, D), jnp.float32), -6.0, 6.0)
    return jnp.concatenate([gains, shifts], axis=0).astype(jnp.float32)


def levels(rng, extent, cuts, least, largest):
    loudness = 1.0
    for dim, blocks in cuts:
        heights = jax.random.uniform(jax.random.fold_in(jax.random.fold_in(rng, 6), dim), (blocks,), jnp.float32, least / len(cuts), largest / len(cuts))
        loudness = loudness * jnp.repeat(jnp.exp(heights), extent[dim] // blocks).reshape((-1,) + (1,) * (len(extent) - 1 - dim))
    return loudness


def noise(key, shape, width, limit, cuts=(), kind=jnp.bfloat16):
    array = width * jax.random.normal(key, shape, jnp.float32)
    if cuts:
        array = array * levels(key, shape, cuts, -0.22, 0.18)
    return jnp.clip(array, -limit, limit).astype(kind)


def setup_inputs(seed: int = 0) -> dict:
    key_list = jax.random.split(jax.random.key(seed), 29)
    block_input = noise(key_list[0], (IMAGES, L, D), 1.0, 6.0, ((0, 8), (1, 4)))
    skip_input = noise(key_list[1], (IMAGES, L, D), 1.0, 6.0, ((0, 8), (2, 4)))
    key_keep = draw_key_keep(jax.random.fold_in(key_list[28], 71), 0)
    output_grad = noise(key_list[3], (IMAGES, L, D), 1.0, 6.0, ((0, 8), (1, 4)))
    skip_weight = noise(key_list[4], (2 * D, D), (2 * D) ** -0.5, 0.125, ((0, 4), (1, 8)), jnp.float32)
    skip_first = noise(key_list[5], (2 * D, D), (0.255 * TOKENS_ALL ** 0.5), 192.0, ((0, 4), (1, 8)), jnp.float32)
    skip_second = jnp.clip(jnp.exp(math.log(18377.855) - 1.3871932 * jax.random.uniform(key_list[6], (2 * D, D), jnp.float32) ** levels(key_list[6], (2 * D, D), ((0, 4), (1, 8)), -0.2, 0.2)), 4590.336, 18377.855)
    attend_weight = noise(key_list[7], (D, 3 * D), D ** -0.5, 0.1875, ((0, 4), (1, 8)), jnp.float32)
    attend_first = noise(key_list[8], (D, 3 * D), (0.128 * TOKENS_ALL ** 0.5), 96.0, ((0, 4), (1, 8)), jnp.float32)
    attend_second = jnp.clip(jnp.exp(math.log(4590.336) - 1.3848565 * jax.random.uniform(key_list[9], (D, 3 * D), jnp.float32) ** levels(key_list[9], (D, 3 * D), ((0, 4), (1, 8)), -0.2, 0.2)), 1149.2352, 4590.336)
    output_weight = noise(key_list[10], (D, D), (3 * D // L) ** -0.5, 3.5, ((0, 4), (1, 8)), jnp.float32)
    output_first = noise(key_list[11], (D, D), (0.213 * IMAGES ** 0.5), 6.0, ((0, 4), (1, 8)), jnp.float32)
    output_second = jnp.clip(jnp.exp(math.log(12.416) - 1.3862944 * jax.random.uniform(key_list[12], (D, D), jnp.float32) ** levels(key_list[12], (D, D), ((0, 4), (1, 8)), -0.2, 0.2)), 3.104, 12.416)
    expand_weight = noise(key_list[13], (D, FF), D ** -0.5, 0.1875, ((0, 4), (1, 8)), jnp.float32)
    expand_first = noise(key_list[14], (D, FF), (0.05 * TOKENS_ALL ** 0.5), 40.0, ((0, 4), (1, 8)), jnp.float32)
    expand_second = jnp.clip(jnp.exp(math.log(703.4112) - 1.3862944 * jax.random.uniform(key_list[15], (D, FF), jnp.float32) ** levels(key_list[15], (D, FF), ((0, 4), (1, 8)), -0.2, 0.2)), 175.8528, 703.4112)
    reduce_weight = noise(key_list[16], (FF, D), (FF // 2) ** -0.5, 0.125, ((0, 4), (1, 8)), jnp.float32)
    reduce_first = noise(key_list[17], (FF, D), (0.0722 * TOKENS_ALL ** 0.5), 56.0, ((0, 4), (1, 8)), jnp.float32)
    reduce_second = jnp.clip(jnp.exp(math.log(1467.9167) - 1.3874198 * jax.random.uniform(key_list[18], (FF, D), jnp.float32) ** levels(key_list[18], (FF, D), ((0, 4), (1, 8)), -0.2, 0.2)), 366.5664, 1467.9167)
    early_weight = noise(key_list[19], (2, D), 0.05, 0.75, ((1, 8),), jnp.float32)
    early_first = noise(key_list[20], (2, D), (0.133 * (D * TOKENS_ALL) ** 0.5 * (3 * D // L) ** -0.5), 2048.0, ((1, 8),), jnp.float32)
    early_second = jnp.clip(jnp.exp(math.log(1921204.2) - 1.3856345 * jax.random.uniform(key_list[21], (2, D), jnp.float32) ** levels(key_list[21], (2, D), ((1, 8),), -0.2, 0.2)), 480618.1, 1921204.2)
    later_weight = draw_later_weight(jax.random.fold_in(key_list[28], 71), 0)
    later_first = noise(key_list[23], (5, D), (0.1665 * TOKENS_ALL ** 0.5), 128.0, ((1, 8),), jnp.float32)
    later_second = jnp.clip(jnp.exp(math.log(7810.176) - 1.3884107 * jax.random.uniform(key_list[24], (5, D), jnp.float32) ** levels(key_list[24], (5, D), ((1, 8),), -0.2, 0.2)), 1948.416, 7810.176)
    hidden_weight = noise(key_list[25], (1, FF), 0.5, 6.0, ((1, 8),), jnp.float32)
    hidden_first = noise(key_list[26], (1, FF), (0.05 * TOKENS_ALL ** 0.5), 40.0, ((1, 8),), jnp.float32)
    hidden_second = jnp.clip(jnp.exp(math.log(703.4112) - 1.3862944 * jax.random.uniform(key_list[27], (1, FF), jnp.float32) ** levels(key_list[27], (1, FF), ((1, 8),), -0.2, 0.2)), 175.8528, 703.4112)
    return dict(block_input=block_input, skip_input=skip_input, key_keep=key_keep, output_grad=output_grad, skip_weight=skip_weight, skip_first=skip_first, skip_second=skip_second, attend_weight=attend_weight, attend_first=attend_first, attend_second=attend_second, output_weight=output_weight, output_first=output_first, output_second=output_second, expand_weight=expand_weight, expand_first=expand_first, expand_second=expand_second, reduce_weight=reduce_weight, reduce_first=reduce_first, reduce_second=reduce_second, early_weight=early_weight, early_first=early_first, early_second=early_second, later_weight=later_weight, later_first=later_first, later_second=later_second, hidden_weight=hidden_weight, hidden_first=hidden_first, hidden_second=hidden_second)


norm_eps = 1e-05
beta_first = 0.9
beta_second = 0.95
adam_eps = 1e-08
decay_rate = 0.1
adam_count = 5.0
masked_score = -1e+30
inverse_root = 0.7071067811865476
step_rates = (0.05, 0.075, 1.5, 0.075, 0.05, 0.1, 0.4, 1.25)

@jax.custom_vjp
def low(v):
    return lax.optimization_barrier(v.astype(jnp.bfloat16)).astype(jnp.float32)

@jax.custom_vjp
def low_back(v):
    return v

def low_keep(v):
    return (low(v), None)

def low_pass(kept, grad):
    return (grad,)

def back_keep(v):
    return (v, None)

def back_low(kept, grad):
    return (low(grad),)
low.defvjp(low_keep, low_pass)
low_back.defvjp(back_keep, back_low)

def matmul(left, right):
    return jnp.dot(left, right, precision=lax.Precision.HIGHEST, preferred_element_type=jnp.float32)

def layer_norm(values, scale_row, shift_row):
    average = lax.optimization_barrier(jnp.mean(values, axis=-1, keepdims=True))
    centred = values - average
    variance = lax.optimization_barrier(jnp.mean(centred * centred, axis=-1, keepdims=True))
    return centred * lax.rsqrt(variance + norm_eps) * scale_row + shift_row

def gelu_exact(values):
    return 0.5 * values * (1.0 + lax.erf(values * inverse_root))

def attend_image(pieces):
    query_rows, key_rows, value_rows, keep_row = pieces
    head_query = query_rows.reshape(L, H, HD)
    head_key = key_rows.reshape(L, H, HD)
    head_value = value_rows.reshape(L, H, HD)
    scores = jnp.einsum('qhd,khd->hqk', head_query, head_key, precision=lax.Precision.HIGHEST) * HD ** (-0.5)
    scores = jnp.where(keep_row[None, None, :] > 0, low_back(scores), masked_score)
    peak_row = lax.optimization_barrier(jnp.max(scores, axis=-1, keepdims=True))
    powers = jnp.exp(scores - peak_row)
    softmax_full = powers / lax.optimization_barrier(jnp.sum(powers, axis=-1, keepdims=True))
    blended = jnp.einsum('hqk,khd->qhd', low(softmax_full), head_value, precision=lax.Precision.HIGHEST)
    return blended.reshape(L, H * HD)

def forward(weights, inputs, skipped, key_keep):
    skip_low, attend_low, output_low, expand_low, reduce_low, early_low, later_low, hidden_low = [low(weight_item) for weight_item in weights]
    joined = jnp.concatenate([inputs, skipped], axis=1)
    merged = low_back(matmul(joined, skip_low) + early_low[1])
    normed_one = layer_norm(merged, later_low[0], early_low[0])
    project = low(low_back(matmul(low(normed_one), attend_low)))
    blocks = project.reshape(IMAGES, L, 3 * D)
    attended = lax.map(jax.checkpoint(attend_image), (blocks[:, :, :D], blocks[:, :, D:2 * D], blocks[:, :, 2 * D:], key_keep))
    attended = low(low_back(attended.reshape(IMAGES * L, D)))
    middle = merged + low_back(matmul(attended, output_low) + later_low[3])
    normed_two = layer_norm(middle, later_low[1], later_low[2])
    hidden_pre = low_back(matmul(low(normed_two), expand_low) + hidden_low[0])
    activated = low(gelu_exact(hidden_pre))
    return middle + low_back(matmul(activated, reduce_low) + later_low[4])

def adamw_update(weight, first_old, second_old, gradient, step_rate):
    moment = beta_first * first_old + (1.0 - beta_first) * gradient
    square = beta_second * second_old + (1.0 - beta_second) * gradient * gradient
    scaled_first = moment / (1.0 - beta_first ** adam_count)
    scaled_second = square / (1.0 - beta_second ** adam_count)
    master = weight - step_rate * (scaled_first / (jnp.sqrt(scaled_second) + adam_eps) + decay_rate * weight)
    return (master, moment, square, master.astype(jnp.bfloat16))

def reference(block_input, skip_input, key_keep, output_grad, skip_weight, skip_first, skip_second, attend_weight, attend_first, attend_second, output_weight, output_first, output_second, expand_weight, expand_first, expand_second, reduce_weight, reduce_first, reduce_second, early_weight, early_first, early_second, later_weight, later_first, later_second, hidden_weight, hidden_first, hidden_second):
    params = (skip_weight, attend_weight, output_weight, expand_weight, reduce_weight, early_weight, later_weight, hidden_weight)
    firsts = (skip_first, attend_first, output_first, expand_first, reduce_first, early_first, later_first, hidden_first)
    seconds = (skip_second, attend_second, output_second, expand_second, reduce_second, early_second, later_second, hidden_second)
    flat_input = block_input.astype(jnp.float32).reshape(IMAGES * L, D)
    flat_skip = skip_input.astype(jnp.float32).reshape(IMAGES * L, D)

    def wrapped(weights, inputs, skipped):
        return forward(weights, inputs, skipped, key_keep)
    result, pullback = jax.vjp(wrapped, params, flat_input, flat_skip)
    weight_grads, input_grad, skip_grad = pullback(output_grad.astype(jnp.float32).reshape(IMAGES * L, D))
    outputs = [result.astype(jnp.bfloat16).reshape(IMAGES, L, D), input_grad.astype(jnp.bfloat16).reshape(IMAGES, L, D), skip_grad.astype(jnp.bfloat16).reshape(IMAGES, L, D)]
    for index_param in range(8):
        outputs.extend(adamw_update(params[index_param], firsts[index_param], seconds[index_param], weight_grads[index_param], step_rates[index_param]))
    return tuple(outputs)
```

```python
import functools
import math

import jax
import jax.numpy as jnp
from jax import lax
from jax.experimental import pallas as pl
from jax.experimental.pallas import tpu as pltpu
from jax.sharding import PartitionSpec as P

H = 16
HD = 72
LANES = 128

norm_eps = 1e-05
beta_first = 0.9
beta_second = 0.95
adam_eps = 1e-08
decay_rate = 0.1
adam_count = 5.0
masked_score = -1e30
inverse_root = 0.7071067811865476
step_rates = (0.05, 0.075, 1.5, 0.075, 0.05, 0.1, 0.4, 1.25)


def layer_norm(values, scale_row, shift_row):
    average = jnp.mean(values, axis=-1, keepdims=True)
    centred = values - average
    variance = jnp.mean(centred * centred, axis=-1, keepdims=True)
    return centred * lax.rsqrt(variance + norm_eps) * scale_row + shift_row


def gelu_exact(values):
    return 0.5 * values * (1.0 + lax.erf(values * inverse_root))


def matmul(left, right, left_dim, right_dim):
    return lax.dot_general(
        left,
        right,
        (((left_dim,), (right_dim,)), ((), ())),
        preferred_element_type=jnp.float32,
    )


def adamw_update(weight, first_old, second_old, gradient, step_rate):
    moment = beta_first * first_old + (1.0 - beta_first) * gradient
    square = beta_second * second_old + (1.0 - beta_second) * gradient * gradient
    scaled_first = moment / (1.0 - beta_first**adam_count)
    scaled_second = square / (1.0 - beta_second**adam_count)
    master = weight - step_rate * (
        scaled_first / (jnp.sqrt(scaled_second) + adam_eps) + decay_rate * weight
    )
    return (master, moment, square, master.astype(jnp.bfloat16))


def round_up(count, step):
    return (count + step - 1) // step * step


def store_heads(source, column, target, row, rows):
    for head in range(H):
        piece = source[:, column + head * HD : column + (head + 1) * HD]
        target[head, row : row + rows, :HD] = piece


def attend_forward_kernel(project, sibling, mask, out, query, key, value, blended):
    rows = project.shape[0]
    gap = round_up(rows, 16)
    width = H * HD
    query[...] = jnp.zeros_like(query)
    key[...] = jnp.zeros_like(key)
    value[...] = jnp.zeros_like(value)
    store_heads(project, 0, query, 0, rows)
    store_heads(project, width, key, 0, rows)
    store_heads(project, 2 * width, value, 0, rows)
    store_heads(sibling, 0, key, gap, rows)
    store_heads(sibling, width, value, gap, rows)
    factor = HD ** (-0.5) * math.log2(math.e)
    keep = mask[...] > 0

    def one_head(head, carry):
        scores = matmul(query[head], key[head], 1, 1)
        scores = jnp.where(keep, scores, masked_score)
        peak = jnp.max(scores, axis=-1, keepdims=True)
        powers = jnp.exp2((scores - peak) * factor)
        totals = jnp.sum(powers, axis=-1, keepdims=True)
        mixed = matmul(powers.astype(jnp.bfloat16), value[head], 1, 0)
        blended[head] = (mixed / totals).astype(jnp.bfloat16)
        return carry

    lax.fori_loop(0, H, one_head, 0)
    for head in range(H):
        out[:, head * HD : (head + 1) * HD] = blended[head, :rows, :HD]


def attend_forward(project, sibling, mask):
    rows, width = project.shape[0], H * HD
    gap = round_up(rows, 16)
    return pl.pallas_call(
        attend_forward_kernel,
        out_shape=jax.ShapeDtypeStruct((rows, width), jnp.bfloat16),
        scratch_shapes=[
            pltpu.VMEM((H, gap, LANES), jnp.bfloat16),
            pltpu.VMEM((H, 2 * gap, LANES), jnp.bfloat16),
            pltpu.VMEM((H, 2 * gap, LANES), jnp.bfloat16),
            pltpu.VMEM((H, gap, LANES), jnp.bfloat16),
        ],
        compiler_params=pltpu.CompilerParams(vmem_limit_bytes=60 << 20),
        cost_estimate=pl.CostEstimate(
            flops=8 * rows * rows * width, bytes_accessed=12 * rows * width, transcendentals=0
        ),
        name="attend_forward",
    )(project, sibling, mask)


def attend_backward_kernel(
    project, sibling, mask, grads, own_grad, sibling_grad, query, key, value, grad, dquery, dkey, dvalue
):
    rows = project.shape[0]
    gap = round_up(rows, 16)
    width = H * HD
    query[...] = jnp.zeros_like(query)
    key[...] = jnp.zeros_like(key)
    value[...] = jnp.zeros_like(value)
    grad[...] = jnp.zeros_like(grad)
    store_heads(project, 0, query, 0, rows)
    store_heads(project, width, key, 0, rows)
    store_heads(project, 2 * width, value, 0, rows)
    store_heads(sibling, 0, key, gap, rows)
    store_heads(sibling, width, value, gap, rows)
    store_heads(grads, 0, grad, 0, rows)
    scale = HD ** (-0.5)
    factor = scale * math.log2(math.e)
    keep = mask[...] > 0

    def one_head(head, carry):
        scores = matmul(key[head], query[head], 1, 1)
        scores = jnp.where(keep, scores, masked_score)
        peak = jnp.max(scores, axis=0, keepdims=True)
        powers = jnp.exp2((scores - peak) * factor)
        totals = jnp.sum(powers, axis=0, keepdims=True)
        probs = powers * (1.0 / totals)
        prob_grad = matmul(value[head], grad[head], 1, 1)
        weighted = probs * prob_grad
        delta = jnp.sum(weighted, axis=0, keepdims=True)
        score_grad = (weighted - probs * delta).astype(jnp.bfloat16)
        dvalue[head] = matmul(probs.astype(jnp.bfloat16), grad[head], 1, 0).astype(jnp.bfloat16)
        dkey[head] = (matmul(score_grad, query[head], 1, 0) * scale).astype(jnp.bfloat16)
        flipped = matmul(key[head].T, score_grad, 1, 0) * scale
        dquery[head] = flipped.T.astype(jnp.bfloat16)
        return carry

    lax.fori_loop(0, H, one_head, 0)
    for head in range(H):
        left, right = head * HD, (head + 1) * HD
        own_grad[:, left:right] = dquery[head, :rows, :HD]
        own_grad[:, width + left : width + right] = dkey[head, :rows, :HD]
        own_grad[:, 2 * width + left : 2 * width + right] = dvalue[head, :rows, :HD]
        sibling_grad[:, left:right] = dkey[head, gap : gap + rows, :HD]
        sibling_grad[:, width + left : width + right] = dvalue[head, gap : gap + rows, :HD]


def attend_backward(project, sibling, mask, grads):
    rows, width = project.shape[0], H * HD
    gap = round_up(rows, 16)
    return pl.pallas_call(
        attend_backward_kernel,
        out_shape=(
            jax.ShapeDtypeStruct((rows, 3 * width), jnp.bfloat16),
            jax.ShapeDtypeStruct((rows, 2 * width), jnp.bfloat16),
        ),
        scratch_shapes=[
            pltpu.VMEM((H, gap, LANES), jnp.bfloat16),
            pltpu.VMEM((H, 2 * gap, LANES), jnp.bfloat16),
            pltpu.VMEM((H, 2 * gap, LANES), jnp.bfloat16),
            pltpu.VMEM((H, gap, LANES), jnp.bfloat16),
            pltpu.VMEM((H, gap, LANES), jnp.bfloat16),
            pltpu.VMEM((H, 2 * gap, LANES), jnp.bfloat16),
            pltpu.VMEM((H, 2 * gap, LANES), jnp.bfloat16),
        ],
        compiler_params=pltpu.CompilerParams(vmem_limit_bytes=60 << 20),
        cost_estimate=pl.CostEstimate(
            flops=20 * rows * rows * width, bytes_accessed=24 * rows * width, transcendentals=0
        ),
        name="attend_backward",
    )(project, sibling, mask, grads)


def merge_kernel(cuts, bit_ref, mine, theirs, *outs):
    half = pl.program_id(1)

    def put(source):
        for (top, bottom, left, right), out in zip(cuts, outs):
            out[0, 0] = source[0, top:bottom, left:right]

    @pl.when(half == bit_ref[0])
    def _():
        put(mine)

    @pl.when(half != bit_ref[0])
    def _():
        put(theirs)


def merge(mine, theirs, bit, cuts=None):
    outer, rows, lanes = mine.shape
    if cuts is None:
        cuts = ((0, rows, 0, lanes),)

    def place(own_bit, index):
        block, half, bit_ref = index
        bit = bit_ref[0] if own_bit else 1 - bit_ref[0]
        return (block, 0, 0)

    outs = pl.pallas_call(
        functools.partial(merge_kernel, cuts),
        grid_spec=pltpu.PrefetchScalarGridSpec(
            num_scalar_prefetch=1,
            grid=(outer, 2),
            in_specs=[
                pl.BlockSpec((1, rows, lanes), lambda o, h, b: (o, 0, 0)),
                pl.BlockSpec((1, rows, lanes), lambda o, h, b: (o, 0, 0)),
            ],
            out_specs=[
                pl.BlockSpec((1, 1, low - top, right - left), lambda o, h, b: (o, h, 0, 0))
                for top, low, left, right in cuts
            ],
        ),
        out_shape=[
            jax.ShapeDtypeStruct((outer, 2, low - top, right - left), mine.dtype)
            for top, low, left, right in cuts
        ],
        compiler_params=pltpu.CompilerParams(vmem_limit_bytes=24 << 20),
        cost_estimate=pl.CostEstimate(
            flops=0, bytes_accessed=8 * outer * rows * lanes, transcendentals=0
        ),
        name="merge",
    )(bit.reshape(1), mine, theirs)
    return outs


def shards(
    sizes,
    block_input,
    skip_input,
    key_keep,
    output_grad,
    skip_weight,
    skip_first,
    skip_second,
    attend_weight,
    attend_first,
    attend_second,
    output_weight,
    output_first,
    output_second,
    expand_weight,
    expand_first,
    expand_second,
    reduce_weight,
    reduce_first,
    reduce_second,
    early_weight,
    early_first,
    early_second,
    later_weight,
    later_first,
    later_second,
    hidden_weight,
    hidden_first,
    hidden_second,
):
    dp, seq = sizes
    bits = dp.bit_length() - 1
    images, local_len, features = block_input.shape
    image_len = skip_input.shape[1]
    tokens = images * local_len
    here = lax.axis_index("dp")
    depth = lax.axis_index("seq")
    core = here % 2
    low = jnp.bfloat16
    columns = features // dp
    depth_rows = features // seq
    hidden_width = hidden_weight.shape[1] * dp

    def swap(values, bit):
        return lax.ppermute(values, "dp", [(i, i ^ (1 << bit)) for i in range(dp)])

    def pick(values, index, axis=0):
        return lax.dynamic_index_in_dim(values, index, axis, keepdims=False)


    def token_pairs(turn):
        pairs = []
        for d in range(dp):
            for z in range(seq):
                line, c = d // 2, d % 2
                to = (line * 2 + z // images) * seq + c * images + (z + turn) % images
                pairs.append((d * seq + z, to))
        return pairs

    def feature_pairs(turn):
        pairs = []
        for d in range(dp):
            for z in range(seq):
                line, c = d // 2, d % 2
                m = (z + turn) % seq
                to = (line * 2 + m // images) * seq + c * images + m % images
                pairs.append((d * seq + z, to))
        return pairs

    def back(pairs):
        return [(b, a) for a, b in pairs]

    both = ("dp", "seq")

    def tokens_in(values):
        pieces = jnp.stack(
            [
                lax.ppermute(pick(values, (depth + r) % images), both, token_pairs(r))
                for r in range(images)
            ]
        )
        order = (depth - jnp.arange(images)) % images
        return jnp.concatenate([pick(pieces, order[q]) for q in range(images)], axis=0)

    def tokens_out(values):
        split = values.reshape(images, local_len, features)
        pieces = jnp.stack(
            [
                lax.ppermute(pick(split, (depth - r) % images), both, back(token_pairs(r)))
                for r in range(images)
            ]
        )
        return jnp.stack([pick(pieces, (j - depth) % images) for j in range(images)])

    def features_in(values):
        split = values.reshape(images, 2, image_len // 2, values.shape[2])
        pieces = []
        for r in range(seq):
            m = (depth + r) % seq
            piece = pick(pick(split, m % images), m // images)
            pieces.append(lax.ppermute(piece, both, feature_pairs(r)))
        pieces = jnp.stack(pieces)
        base = core * images + depth % images
        return jnp.concatenate([pick(pieces, (base - s) % seq) for s in range(seq)], axis=1)

    def features_out(values):
        split = values.reshape(tokens, seq, features // seq).transpose(1, 0, 2)
        base = core * images + depth % images
        pieces = jnp.stack(
            [
                lax.ppermute(pick(split, (base - r) % seq), both, back(feature_pairs(r)))
                for r in range(seq)
            ]
        )
        rows = []
        for j in range(images):
            rows.append(
                jnp.concatenate(
                    [pick(pieces, (c * images + j - depth) % seq) for c in range(2)], axis=0
                )
            )
        return jnp.stack(rows)


    def flip(weight):
        rows, width = weight.shape
        return weight.astype(low).reshape(rows, width // columns, columns).transpose(2, 1, 0)

    def lanes_of(flipped):
        return flipped.reshape(columns, flipped.shape[1] * flipped.shape[2])

    small = jnp.concatenate(
        [early_weight, later_weight, hidden_weight.reshape(-1, columns)], axis=0
    ).astype(low)
    small_count = small.shape[0]
    small_lanes = round_up(small_count, 64)
    small_flipped = jnp.pad(small.T, ((0, 0), (0, small_lanes - small_count)))

    def gather_depth(shard):
        pieces = [shard]
        for r in range(1, seq):
            pieces.append(
                lax.ppermute(shard, "seq", [(z, (z + r) % seq) for z in range(seq)])
            )
        stacked = jnp.stack(pieces)
        return [pick(stacked, (depth - s) % seq) for s in range(seq)]

    def join_depth(pieces, start, count, width):
        rows = []
        for a in range(count):
            left = start + a * width
            rows.append(jnp.concatenate([p[:, left : left + width] for p in pieces], axis=1))
        return jnp.concatenate(rows, axis=0) if count > 1 else rows[0]

    def gather_dp(shard, order, cuts=None):
        rows, lanes = shard.shape
        current = shard[None]
        held = []
        for step, bit in enumerate(order):
            other = swap(current, bit)
            inner = 1
            for done in held:
                if done < bit:
                    inner *= 2
            outer = current.shape[0] // inner
            mine_bit = (here >> bit) & 1
            last = step == len(order) - 1
            merged_parts = merge(
                current.reshape(outer, inner * rows, lanes),
                other.reshape(outer, inner * rows, lanes),
                mine_bit,
                cuts if last else None,
            )
            held.append(bit)
            if last:
                return [part.reshape(dp, -1, part.shape[-1]) for part in merged_parts]
            current = merged_parts[0].reshape(-1, rows, lanes)

    outer_bits = list(range(1, bits))
    first_order = outer_bits + [0]
    second_order = outer_bits[::-1] + [0]

    skip_width = skip_weight.shape[0]
    reduce_width = reduce_weight.shape[0]

    pieces = gather_depth(jnp.concatenate([lanes_of(flip(skip_weight)), small_flipped], axis=1))
    skip_shard = jnp.concatenate(
        [
            join_depth(pieces, 0, 1, skip_width),
            jnp.pad(pieces[0][:, skip_width:], ((0, 0), (0, LANES - small_lanes))),
        ],
        axis=1,
    )
    skip_lanes = seq * skip_width
    skip_full, small_full = gather_dp(
        skip_shard,
        first_order,
        ((0, columns, 0, skip_lanes), (0, columns, skip_lanes, skip_lanes + LANES)),
    )
    skip_full = skip_full.reshape(features, skip_lanes)

    attend_count = attend_weight.shape[1] // columns
    pieces = gather_depth(
        jnp.concatenate([lanes_of(flip(attend_weight)), lanes_of(flip(output_weight))], axis=1)
    )
    attend_full, output_full = gather_dp(
        join_depth(pieces, 0, attend_count + 1, depth_rows),
        second_order,
        (
            (0, attend_count * columns, 0, features),
            (attend_count * columns, (attend_count + 1) * columns, 0, features),
        ),
    )
    attend_full = attend_full.reshape(3 * features, features)
    output_full = output_full.reshape(features, features)

    expand_count = expand_weight.shape[1] // columns
    pieces = gather_depth(lanes_of(flip(expand_weight)))
    expand_full = gather_dp(join_depth(pieces, 0, expand_count, depth_rows), first_order)[0]
    expand_full = expand_full.reshape(hidden_width, features)

    pieces = gather_depth(lanes_of(flip(reduce_weight)))
    reduce_full = gather_dp(join_depth(pieces, 0, 1, reduce_width), second_order)[0]
    reduce_full = reduce_full.reshape(features, hidden_width)

    small_rows = small_full[:, :, :small_count].astype(jnp.float32)
    early_row = small_rows[:, :, :2].reshape(features, 2).T
    later_row = small_rows[:, :, 2:7].reshape(features, 5).T
    hidden_row = small_rows[:, :, 7:].transpose(0, 2, 1).reshape(hidden_width)


    inputs = jnp.concatenate([tokens_in(block_input), features_in(skip_input)], axis=1)
    grad_out = tokens_in(output_grad)

    line_keep = jnp.stack([key_keep, swap(key_keep, 0)])
    line_keep = jnp.concatenate([pick(line_keep, core), pick(line_keep, 1 - core)], axis=0)
    image_keep = pick(line_keep, depth).reshape(2, tokens)
    gap = round_up(tokens, 16)
    pads = jnp.zeros((gap - tokens,), jnp.int32)
    mask = jnp.concatenate([pick(image_keep, core), pads, pick(image_keep, 1 - core), pads])


    merged = matmul(inputs, skip_full, 1, 1) + early_row[1]
    normed_one, norm_one_back = jax.vjp(layer_norm, merged, later_row[0], early_row[0])
    normed_one_low = normed_one.astype(low)
    project = matmul(normed_one_low, attend_full, 1, 1).astype(low)
    sibling = swap(project[:, features:], 0)
    attended_low = attend_forward(project, sibling, mask[None, :])
    middle = merged + matmul(attended_low, output_full, 1, 1) + later_row[3]
    normed_two, norm_two_back = jax.vjp(layer_norm, middle, later_row[1], later_row[2])
    normed_two_low = normed_two.astype(low)
    hidden_pre = matmul(normed_two_low, expand_full, 1, 1) + hidden_row
    activated, gelu_back = jax.vjp(gelu_exact, hidden_pre)
    activated_low = activated.astype(low)
    block_output = (middle + matmul(activated_low, reduce_full, 1, 1) + later_row[4]).astype(low)
    block_output = tokens_out(block_output)


    def scatter_dp(gradient, order):
        lanes = gradient.shape[1]
        current = gradient.reshape([2] * bits + [-1, lanes])
        held = list(range(bits))[::-1]
        for bit in order:
            axis = held.index(bit)
            mine_bit = (here >> bit) & 1
            arrived = swap(pick(current, 1 - mine_bit, axis), bit)
            kept = pick(current, mine_bit, axis)
            current = (kept.astype(jnp.float32) + arrived.astype(jnp.float32)).astype(low)
            held.remove(bit)
        return current

    def scatter_depth(chunks):
        total = pick(chunks, depth).astype(jnp.float32)
        for r in range(1, seq):
            arrived = lax.ppermute(
                pick(chunks, (depth + r) % seq), "seq", [(z, (z + r) % seq) for z in range(seq)]
            )
            total = total + arrived.astype(jnp.float32)
        return total

    def split_depth(summed, count):
        rows, lanes = summed.shape
        width = lanes // seq
        parts = summed.reshape(count, columns, seq, width).transpose(2, 1, 0, 3)
        return parts.reshape(seq, columns, count * width)

    def unflip(total, count):
        width = total.shape[1] // count
        return total.reshape(columns, count, width).transpose(2, 1, 0).reshape(width, -1)

    back_first = [0] + outer_bits
    back_second = [0] + outer_bits[::-1]


    grad_out_full = grad_out.astype(jnp.float32)
    reduce_grad = matmul(grad_out, activated_low, 0, 0).astype(low)
    reduce_total = unflip(scatter_depth(split_depth(scatter_dp(reduce_grad, back_first), 1)), 1)

    grad_act = matmul(grad_out, reduce_full, 1, 0)
    grad_pre_low = gelu_back(grad_act)[0].astype(low)
    expand_grad = matmul(grad_pre_low, normed_two_low, 0, 0).astype(low)
    expand_total = unflip(
        scatter_depth(split_depth(scatter_dp(expand_grad, back_second), expand_count)),
        expand_count,
    )
    hidden_grad = jnp.sum(grad_pre_low.astype(jnp.float32), axis=0)
    grad_normed_two = matmul(grad_pre_low, expand_full, 1, 0)
    grad_middle_part, gain_two_grad, shift_two_grad = norm_two_back(grad_normed_two)
    grad_middle = grad_out_full + grad_middle_part
    grad_branch_low = grad_middle.astype(low)
    output_weight_grad = matmul(grad_branch_low, attended_low, 0, 0).astype(low)
    output_total = unflip(
        scatter_depth(split_depth(scatter_dp(output_weight_grad, back_first), 1)), 1
    )
    grad_attended = matmul(grad_branch_low, output_full, 1, 0).astype(low)
    own_grad, sibling_grad = attend_backward(project, sibling, mask[:, None], grad_attended)
    returned = swap(sibling_grad, 0)
    project_grad = jnp.concatenate(
        [
            own_grad[:, :features],
            (
                own_grad[:, features:].astype(jnp.float32) + returned.astype(jnp.float32)
            ).astype(low),
        ],
        axis=1,
    )
    attend_grad = matmul(project_grad, normed_one_low, 0, 0).astype(low)
    attend_total = unflip(
        scatter_depth(split_depth(scatter_dp(attend_grad, back_second), attend_count)),
        attend_count,
    )
    grad_normed_one = matmul(project_grad, attend_full, 1, 0)
    grad_merged_part, gain_one_grad, shift_one_grad = norm_one_back(grad_normed_one)
    grad_merged_low = (grad_middle + grad_merged_part).astype(low)
    skip_grad_weight = matmul(grad_merged_low, inputs, 0, 0).astype(low)

    small_grad = jnp.concatenate(
        [
            jnp.stack(
                [
                    shift_one_grad,
                    jnp.sum(grad_merged_low.astype(jnp.float32), axis=0),
                    gain_one_grad,
                    gain_two_grad,
                    shift_two_grad,
                    jnp.sum(grad_branch_low.astype(jnp.float32), axis=0),
                    jnp.sum(grad_out_full, axis=0),
                ]
            ),
            hidden_grad.reshape(dp, -1, columns).transpose(1, 0, 2).reshape(-1, features),
        ],
        axis=0,
    ).astype(low)
    small_grad = jnp.pad(small_grad.T, ((0, 0), (0, LANES - small_count)))
    summed = scatter_dp(jnp.concatenate([skip_grad_weight, small_grad], axis=1), back_first)
    skip_chunks = split_depth(summed[:, :skip_lanes], 1)
    small_chunks = jnp.broadcast_to(
        summed[None, :, skip_lanes : skip_lanes + small_lanes], (seq, columns, small_lanes)
    )
    total = scatter_depth(jnp.concatenate([skip_chunks, small_chunks], axis=2))
    skip_total = unflip(total[:, :skip_width], 1)
    small_total = total[:, skip_width : skip_width + small_count].T
    early_total = small_total[:2]
    later_total = small_total[2:7]
    hidden_total = small_total[7:].reshape(1, -1)

    grad_inputs = matmul(grad_merged_low, skip_full, 1, 0).astype(low)
    input_grad = tokens_out(grad_inputs[:, :features])
    skip_grad = features_out(grad_inputs[:, features:])

    results = [block_output, input_grad, skip_grad]
    results.extend(adamw_update(skip_weight, skip_first, skip_second, skip_total, step_rates[0]))
    results.extend(
        adamw_update(attend_weight, attend_first, attend_second, attend_total, step_rates[1])
    )
    results.extend(
        adamw_update(output_weight, output_first, output_second, output_total, step_rates[2])
    )
    results.extend(
        adamw_update(expand_weight, expand_first, expand_second, expand_total, step_rates[3])
    )
    results.extend(
        adamw_update(reduce_weight, reduce_first, reduce_second, reduce_total, step_rates[4])
    )
    results.extend(
        adamw_update(early_weight, early_first, early_second, early_total, step_rates[5])
    )
    results.extend(
        adamw_update(later_weight, later_first, later_second, later_total, step_rates[6])
    )
    results.extend(
        adamw_update(hidden_weight, hidden_first, hidden_second, hidden_total, step_rates[7])
    )
    return tuple(results)


def solution(mesh):
    sizes = (mesh.shape["dp"], mesh.shape["seq"])
    matrix, row = P("seq", "dp"), P(None, "dp")
    token, feature = P("dp", "seq", None), P("dp", None, "seq")
    return jax.shard_map(
        functools.partial(shards, sizes),
        mesh=mesh,
        in_specs=(token, feature, P("dp", None), token) + (matrix,) * 15 + (row,) * 9,
        out_specs=(token, token, feature) + (matrix,) * 20 + (row,) * 12,
        check_vma=False,
    )
```

```python
import functools
import math

import jax
import jax.numpy as jnp
from jax import lax
from jax.experimental import pallas as pl
from jax.experimental.pallas import tpu as pltpu
from jax.sharding import PartitionSpec as P

H = 16
HD = 72
LANES = 128

norm_eps = 1e-05
beta_first = 0.9
beta_second = 0.95
adam_eps = 1e-08
decay_rate = 0.1
adam_count = 5.0
masked_score = -1e30
inverse_root = 0.7071067811865476
step_rates = (0.05, 0.075, 1.5, 0.075, 0.05, 0.1, 0.4, 1.25)


def layer_norm(values, scale_row, shift_row):
    average = jnp.mean(values, axis=-1, keepdims=True)
    centred = values - average
    variance = jnp.mean(centred * centred, axis=-1, keepdims=True)
    return centred * lax.rsqrt(variance + norm_eps) * scale_row + shift_row


def gelu_exact(values):
    return 0.5 * values * (1.0 + lax.erf(values * inverse_root))


def matmul(left, right, left_dim, right_dim):
    return lax.dot_general(
        left,
        right,
        (((left_dim,), (right_dim,)), ((), ())),
        preferred_element_type=jnp.float32,
    )


def adamw_update(weight, first_old, second_old, gradient, step_rate):
    moment = beta_first * first_old + (1.0 - beta_first) * gradient
    square = beta_second * second_old + (1.0 - beta_second) * gradient * gradient
    scaled_first = moment / (1.0 - beta_first**adam_count)
    scaled_second = square / (1.0 - beta_second**adam_count)
    master = weight - step_rate * (
        scaled_first / (jnp.sqrt(scaled_second) + adam_eps) + decay_rate * weight
    )
    return (master, moment, square, master.astype(jnp.bfloat16))


def round_up(count, step):
    return (count + step - 1) // step * step


def store_heads(source, column, target, row, rows):
    for head in range(H):
        piece = source[:, column + head * HD : column + (head + 1) * HD]
        target[head, row : row + rows, :HD] = piece


def attend_forward_kernel(project, sibling, mask, out, query, key, value, blended):
    rows = project.shape[0]
    gap = round_up(rows, 16)
    width = H * HD
    query[...] = jnp.zeros_like(query)
    key[...] = jnp.zeros_like(key)
    value[...] = jnp.zeros_like(value)
    store_heads(project, 0, query, 0, rows)
    store_heads(project, width, key, 0, rows)
    store_heads(project, 2 * width, value, 0, rows)
    store_heads(sibling, 0, key, gap, rows)
    store_heads(sibling, width, value, gap, rows)
    factor = HD ** (-0.5) * math.log2(math.e)
    keep = mask[...] > 0

    def one_head(head, carry):
        scores = matmul(query[head], key[head], 1, 1)
        scores = jnp.where(keep, scores, masked_score)
        peak = jnp.max(scores, axis=-1, keepdims=True)
        powers = jnp.exp2((scores - peak) * factor)
        totals = jnp.sum(powers, axis=-1, keepdims=True)
        mixed = matmul(powers.astype(jnp.bfloat16), value[head], 1, 0)
        blended[head] = (mixed / totals).astype(jnp.bfloat16)
        return carry

    lax.fori_loop(0, H, one_head, 0)
    for head in range(H):
        out[:, head * HD : (head + 1) * HD] = blended[head, :rows, :HD]


def attend_forward(project, sibling, mask):
    rows, width = project.shape[0], H * HD
    gap = round_up(rows, 16)
    return pl.pallas_call(
        attend_forward_kernel,
        out_shape=jax.ShapeDtypeStruct((rows, width), jnp.bfloat16),
        scratch_shapes=[
            pltpu.VMEM((H, gap, LANES), jnp.bfloat16),
            pltpu.VMEM((H, 2 * gap, LANES), jnp.bfloat16),
            pltpu.VMEM((H, 2 * gap, LANES), jnp.bfloat16),
            pltpu.VMEM((H, gap, LANES), jnp.bfloat16),
        ],
        compiler_params=pltpu.CompilerParams(vmem_limit_bytes=60 << 20),
        cost_estimate=pl.CostEstimate(
            flops=8 * rows * rows * width, bytes_accessed=12 * rows * width, transcendentals=0
        ),
        name="attend_forward",
    )(project, sibling, mask)


def attend_backward_kernel(
    project, sibling, mask, grads, own_grad, sibling_grad, query, key, value, grad, dquery, dkey, dvalue
):
    rows = project.shape[0]
    gap = round_up(rows, 16)
    width = H * HD
    query[...] = jnp.zeros_like(query)
    key[...] = jnp.zeros_like(key)
    value[...] = jnp.zeros_like(value)
    grad[...] = jnp.zeros_like(grad)
    store_heads(project, 0, query, 0, rows)
    store_heads(project, width, key, 0, rows)
    store_heads(project, 2 * width, value, 0, rows)
    store_heads(sibling, 0, key, gap, rows)
    store_heads(sibling, width, value, gap, rows)
    store_heads(grads, 0, grad, 0, rows)
    scale = HD ** (-0.5)
    factor = scale * math.log2(math.e)
    keep = mask[...] > 0

    def one_head(head, carry):
        scores = matmul(key[head], query[head], 1, 1)
        scores = jnp.where(keep, scores, masked_score)
        peak = jnp.max(scores, axis=0, keepdims=True)
        powers = jnp.exp2((scores - peak) * factor)
        totals = jnp.sum(powers, axis=0, keepdims=True)
        probs = powers * (1.0 / totals)
        prob_grad = matmul(value[head], grad[head], 1, 1)
        weighted = probs * prob_grad
        delta = jnp.sum(weighted, axis=0, keepdims=True)
        score_grad = (weighted - probs * delta).astype(jnp.bfloat16)
        dvalue[head] = matmul(probs.astype(jnp.bfloat16), grad[head], 1, 0).astype(jnp.bfloat16)
        dkey[head] = (matmul(score_grad, query[head], 1, 0) * scale).astype(jnp.bfloat16)
        flipped = matmul(key[head].T, score_grad, 1, 0) * scale
        dquery[head] = flipped.T.astype(jnp.bfloat16)
        return carry

    lax.fori_loop(0, H, one_head, 0)
    for head in range(H):
        left, right = head * HD, (head + 1) * HD
        own_grad[:, left:right] = dquery[head, :rows, :HD]
        own_grad[:, width + left : width + right] = dkey[head, :rows, :HD]
        own_grad[:, 2 * width + left : 2 * width + right] = dvalue[head, :rows, :HD]
        sibling_grad[:, left:right] = dkey[head, gap : gap + rows, :HD]
        sibling_grad[:, width + left : width + right] = dvalue[head, gap : gap + rows, :HD]


def attend_backward(project, sibling, mask, grads):
    rows, width = project.shape[0], H * HD
    gap = round_up(rows, 16)
    return pl.pallas_call(
        attend_backward_kernel,
        out_shape=(
            jax.ShapeDtypeStruct((rows, 3 * width), jnp.bfloat16),
            jax.ShapeDtypeStruct((rows, 2 * width), jnp.bfloat16),
        ),
        scratch_shapes=[
            pltpu.VMEM((H, gap, LANES), jnp.bfloat16),
            pltpu.VMEM((H, 2 * gap, LANES), jnp.bfloat16),
            pltpu.VMEM((H, 2 * gap, LANES), jnp.bfloat16),
            pltpu.VMEM((H, gap, LANES), jnp.bfloat16),
            pltpu.VMEM((H, gap, LANES), jnp.bfloat16),
            pltpu.VMEM((H, 2 * gap, LANES), jnp.bfloat16),
            pltpu.VMEM((H, 2 * gap, LANES), jnp.bfloat16),
        ],
        compiler_params=pltpu.CompilerParams(vmem_limit_bytes=60 << 20),
        cost_estimate=pl.CostEstimate(
            flops=20 * rows * rows * width, bytes_accessed=24 * rows * width, transcendentals=0
        ),
        name="attend_backward",
    )(project, sibling, mask, grads)


VMEM_SPEC = pl.BlockSpec(memory_space=pltpu.VMEM)
SMEM_SPEC = pl.BlockSpec(memory_space=pltpu.SMEM)


def local_call(kernel, name, info, operands, outs, scratch=(), aliases=None):
    moved = sum(x.size * x.dtype.itemsize for x in operands)
    moved += sum(math.prod(shape) * jnp.dtype(kind).itemsize for shape, kind in outs)
    return pl.pallas_call(
        kernel,
        out_shape=[jax.ShapeDtypeStruct(shape, kind) for shape, kind in outs],
        in_specs=[SMEM_SPEC] + [VMEM_SPEC] * len(operands),
        out_specs=[VMEM_SPEC] * len(outs),
        scratch_shapes=list(scratch),
        compiler_params=pltpu.CompilerParams(vmem_limit_bytes=48 << 20),
        cost_estimate=pl.CostEstimate(flops=0, bytes_accessed=moved, transcendentals=0),
        name=name,
    )(info, *operands)


def insert_bit(combo, place, bit):
    below = combo & ((1 << place) - 1)
    above = combo >> place
    return (above << (place + 1)) + bit * (1 << place) + below


def pack_kernel(counts, small_count, info, *refs):
    weights, small, outs = refs[:5], refs[5], refs[6:]
    skip, attend, output, expand, reduce = weights
    first, second, third, fourth = outs
    low = jnp.bfloat16
    columns = skip.shape[1]
    rows = skip.shape[0]
    first[:, :rows] = skip[...].T.astype(low)
    tail = jnp.concatenate(
        [
            small[...].T.astype(low),
            jnp.zeros((columns, first.shape[1] - rows - small_count), low),
        ],
        axis=1,
    )
    first[:, rows:] = tail

    def spread(weight, out, start):
        rows, width = weight.shape
        flipped = weight[...].T.astype(low)
        for a in range(width // columns):
            left = start + a * rows
            out[:, left : left + rows] = flipped[a * columns : (a + 1) * columns]

    spread(attend, second, 0)
    spread(output, second, attend.shape[0] * (attend.shape[1] // columns))
    spread(expand, third, 0)
    spread(reduce, fourth, 0)


def join_kernel(plan, seq, info, *refs):
    pieces, outs, held = refs[:seq], refs[seq:-1], refs[-1]
    for r in range(seq):
        held[r] = pieces[r][...]
    depth = info[0]
    for s in range(seq):
        piece = held[lax.rem(depth - s + seq, seq)]
        for only, left, width, out, row, lane in plan(s):
            outs[out][row : row + piece.shape[0], lane : lane + width] = piece[
                :, left : left + width
            ]


def tokens_in_kernel(images, seq, info, *refs):
    pieces, features, out = refs[:images], refs[images:-3], refs[-3]
    held, held_features = refs[-2], refs[-1]
    length, width = pieces[0].shape
    for r in range(images):
        held[r] = pieces[r][...]
    for q in range(images):
        out[q * length : (q + 1) * length, :width] = held[lax.rem(info[0] - q + seq, images)]
    if features:
        part = features[0].shape[1]
        for r in range(seq):
            held_features[r] = features[r][...]
        for s in range(seq):
            left = width + s * part
            out[:, left : left + part] = held_features[lax.rem(info[1] - s + seq, seq)]


def tokens_out_kernel(images, seq, info, values, *refs):
    pieces, features = refs[:images], refs[images:-2]
    held, held_features = refs[-2], refs[-1]
    length, width = pieces[0].shape
    for q in range(images):
        held[q] = values[q * length : (q + 1) * length, :width]
    for r in range(images):
        pieces[r][...] = held[lax.rem(info[0] - r + seq, images)]
    if features:
        part = features[0].shape[1]
        for s in range(seq):
            left = width + s * part
            held_features[s] = values[:, left : left + part]
        for r in range(seq):
            features[r][...] = held_features[lax.rem(info[1] - r + seq, seq)]


def merge_kernel(plan, count, bit_ref, *refs):
    mine, theirs, outs = refs[:count], refs[count : 2 * count], refs[2 * count :]
    half = pl.program_id(1)

    def put(sources):
        for source, top, low, left, right, out, row, lane in plan:
            outs[out][0, 0, row : row + low - top, lane : lane + right - left] = sources[source][
                0, top:low, left:right
            ]

    @pl.when(half == bit_ref[0])
    def _():
        put(mine)

    @pl.when(half != bit_ref[0])
    def _():
        put(theirs)


def merge(mine, theirs, bit, plan, outs):
    outer = mine[0].shape[0]
    count = len(mine)
    moved = sum(4 * x.size for x in mine) * 2
    return pl.pallas_call(
        functools.partial(merge_kernel, plan, count),
        grid_spec=pltpu.PrefetchScalarGridSpec(
            num_scalar_prefetch=1,
            grid=(outer, 2),
            in_specs=[
                pl.BlockSpec((1,) + x.shape[1:], lambda o, h, b: (o, 0, 0)) for x in mine + theirs
            ],
            out_specs=[
                pl.BlockSpec((1, 1, rows, lanes), lambda o, h, b: (o, h, 0, 0))
                for rows, lanes in outs
            ],
        ),
        out_shape=[
            jax.ShapeDtypeStruct((outer, 2, rows, lanes), mine[0].dtype) for rows, lanes in outs
        ],
        compiler_params=pltpu.CompilerParams(vmem_limit_bytes=32 << 20),
        cost_estimate=pl.CostEstimate(flops=0, bytes_accessed=moved, transcendentals=0),
        name="merge",
    )(bit.reshape(1), *mine, *theirs)


def carve_kernel(bit_ref, *refs):
    count = len(refs) - 1
    out = refs[-1]
    row = 0
    for source in refs[:count]:
        rows = source.shape[2]
        out[0, row : row + rows] = source[0, 0]
        row += rows


def carve(sources, bit):
    outer, _, _, lanes = sources[0].shape
    rows = sum(x.shape[2] for x in sources)
    return pl.pallas_call(
        carve_kernel,
        grid_spec=pltpu.PrefetchScalarGridSpec(
            num_scalar_prefetch=1,
            grid=(outer,),
            in_specs=[
                pl.BlockSpec((1, 1) + x.shape[2:], lambda o, b: (o, 1 - b[0], 0, 0))
                for x in sources
            ],
            out_specs=pl.BlockSpec((1, rows, lanes), lambda o, b: (o, 0, 0)),
        ),
        out_shape=jax.ShapeDtypeStruct((outer, rows, lanes), sources[0].dtype),
        compiler_params=pltpu.CompilerParams(vmem_limit_bytes=32 << 20),
        cost_estimate=pl.CostEstimate(
            flops=0, bytes_accessed=4 * outer * rows * lanes, transcendentals=0
        ),
        name="carve",
    )(bit.reshape(1), *sources)


def fold_first_kernel(plan, places, count, bit_ref, info, *refs):
    sources, arrived = refs[:count], refs[count]
    outs = refs[count + 1 :]
    outer = arrived.shape[0]
    row = 0
    spans = []
    for index, source in enumerate(sources):
        spans.append((index, row, source.shape[2]))
        row += source.shape[2]
    for half, (place, info_index) in enumerate(places):
        bit = info[info_index]
        top, low, left, right = plan[half]
        for combo in range(outer // 2):
            for kept in range(2):
                at = insert_bit(combo, place, bit if kept == 0 else 1 - bit)
                target = outs[2 * half + kept]
                for index, start, rows in spans:
                    a, b = max(top, start), min(low, start + rows)
                    if a < b:
                        total = sources[index][at, 0, a - start : b - start, left:right].astype(
                            jnp.float32
                        ) + arrived[at, a:b, left:right].astype(jnp.float32)
                        target[combo, a - top : b - top] = total.astype(jnp.bfloat16)


def fold_first(sources, arrived, bit, info, plan, places):
    outer = arrived.shape[0]
    outs = []
    for top, low, left, right in plan:
        outs += [((outer // 2, low - top, right - left), jnp.bfloat16)] * 2
    moved = 4 * arrived.size + sum(2 * math.prod(shape) for shape, _ in outs)
    count = len(sources)
    return pl.pallas_call(
        functools.partial(fold_first_kernel, plan, places, count),
        grid_spec=pltpu.PrefetchScalarGridSpec(
            num_scalar_prefetch=2,
            grid=(1,),
            in_specs=[
                pl.BlockSpec(
                    (outer, 1) + x.shape[2:],
                    lambda i, b, f: (0, b[0], 0, 0),
                    pipeline_mode=pl.Buffered(1),
                )
                for x in sources
            ]
            + [
                pl.BlockSpec(
                    arrived.shape, lambda i, b, f: (0, 0, 0), pipeline_mode=pl.Buffered(1)
                )
            ],
            out_specs=[
                pl.BlockSpec(shape, lambda i, b, f: (0, 0, 0), pipeline_mode=pl.Buffered(1))
                for shape, _ in outs
            ],
        ),
        out_shape=[jax.ShapeDtypeStruct(shape, kind) for shape, kind in outs],
        compiler_params=pltpu.CompilerParams(vmem_limit_bytes=48 << 20),
        cost_estimate=pl.CostEstimate(flops=0, bytes_accessed=moved, transcendentals=0),
        name="fold_first",
    )(bit.reshape(1), info, *sources, arrived)


def fold_next_kernel(places, info, *refs):
    halves = len(places)
    outs = refs[2 * halves :]
    for half, (place, info_index) in enumerate(places):
        kept, arrived = refs[2 * half], refs[2 * half + 1]
        bit = info[info_index]
        for combo in range(kept.shape[0] // 2):
            for side in range(2):
                at = insert_bit(combo, place, bit if side == 0 else 1 - bit)
                total = kept[at].astype(jnp.float32) + arrived[at].astype(jnp.float32)
                outs[2 * half + side][combo] = total.astype(jnp.bfloat16)


def split_kernel(plan, seq, halves, info, *refs):
    outs, held = refs[2 * halves : -1], refs[-1]
    depth = info[0]
    for half in range(halves):
        kept, arrived = refs[2 * half], refs[2 * half + 1]
        total = (kept[0].astype(jnp.float32) + arrived[0].astype(jnp.float32)).astype(jnp.bfloat16)
        for s, row, rows, left, width, lane in plan[half]:
            held[s, :, lane : lane + width] = total[row : row + rows, left : left + width]
    for r in range(seq):
        outs[r][...] = held[lax.rem(depth + r, seq)]


def update(weight, first_old, second_old, gradient, rate, outs):
    results = adamw_update(weight, first_old, second_old, gradient, rate)
    for out, result in zip(outs, results):
        out[...] = result


def adam_kernel(seq, parts, info, *refs):
    pieces = refs[:seq]
    total = pieces[0][...].astype(jnp.float32)
    for piece in pieces[1:]:
        total = total + piece[...].astype(jnp.float32)
    flipped = total.T
    refs = refs[seq:]
    states, outs = refs[: 3 * len(parts)], refs[3 * len(parts) :]
    columns = total.shape[0]
    for index, (start, width, count, rate) in enumerate(parts):
        weight, first_old, second_old = states[3 * index : 3 * index + 3]
        results = outs[4 * index : 4 * index + 4]
        for a in range(count):
            top = start + a * width
            lanes = slice(a * columns, (a + 1) * columns)
            values = adamw_update(
                weight[:, lanes],
                first_old[:, lanes],
                second_old[:, lanes],
                flipped[top : top + width],
                rate,
            )
            for result, value in zip(results, values):
                result[:, lanes] = value


def shards(
    sizes,
    block_input,
    skip_input,
    key_keep,
    output_grad,
    skip_weight,
    skip_first,
    skip_second,
    attend_weight,
    attend_first,
    attend_second,
    output_weight,
    output_first,
    output_second,
    expand_weight,
    expand_first,
    expand_second,
    reduce_weight,
    reduce_first,
    reduce_second,
    early_weight,
    early_first,
    early_second,
    later_weight,
    later_first,
    later_second,
    hidden_weight,
    hidden_first,
    hidden_second,
):
    dp, seq = sizes
    bits = dp.bit_length() - 1
    images, local_len, features = block_input.shape
    image_len, part = skip_input.shape[1:]
    tokens = images * local_len
    here = lax.axis_index("dp")
    depth = lax.axis_index("seq")
    core = here % 2
    base = core * images + depth % images
    info = jnp.stack([depth, base] + [(here >> b) & 1 for b in range(bits)]).astype(jnp.int32)
    low = jnp.bfloat16
    columns = features // dp
    depth_rows = features // seq
    hidden_width = hidden_weight.shape[1] * dp
    outer_bits = list(range(1, bits))
    tie = lax.optimization_barrier

    def swap(values, bit):
        return lax.ppermute(values, "dp", [(i, i ^ (1 << bit)) for i in range(dp)])

    def pick(values, index, axis=0):
        return lax.dynamic_index_in_dim(values, index, axis, keepdims=False)

    def shift(values, r):
        return lax.ppermute(values, "seq", [(z, (z + r) % seq) for z in range(seq)])


    both = ("dp", "seq")

    def token_pairs(turn):
        pairs = []
        for d in range(dp):
            for z in range(seq):
                line, c = d // 2, d % 2
                to = (line * 2 + z // images) * seq + c * images + (z + turn) % images
                pairs.append((d * seq + z, to))
        return pairs

    def feature_pairs(turn):
        pairs = []
        for d in range(dp):
            for z in range(seq):
                line, c = d // 2, d % 2
                m = (z + turn) % seq
                to = (line * 2 + m // images) * seq + c * images + m % images
                pairs.append((d * seq + z, to))
        return pairs

    def back(pairs):
        return [(b, a) for a, b in pairs]

    def token_slices(values):
        return [pick(values, (depth + r) % images) for r in range(images)]

    def feature_slices(values):
        split = values.reshape(images, 2, image_len // 2, part)
        slices = []
        for r in range(seq):
            m = (depth + r) % seq
            slices.append(pick(pick(split, m % images), m // images))
        return slices

    def send_tokens(slices):
        return [lax.ppermute(x, both, token_pairs(r)) for r, x in enumerate(slices)]

    def send_features(slices):
        return [lax.ppermute(x, both, feature_pairs(r)) for r, x in enumerate(slices)]

    def return_tokens(pieces):
        return [lax.ppermute(x, both, back(token_pairs(r))) for r, x in enumerate(pieces)]

    def return_features(pieces):
        return [lax.ppermute(x, both, back(feature_pairs(r))) for r, x in enumerate(pieces)]

    held_tokens = pltpu.VMEM((images, local_len, features), low)
    held_features = pltpu.VMEM((seq, tokens, part), low)

    def join_tokens(pieces, parts=()):
        width = features + len(parts) * part
        return local_call(
            functools.partial(tokens_in_kernel, images, seq),
            "join_tokens",
            info,
            list(pieces) + list(parts),
            [((tokens, width), low)],
            [held_tokens, held_features],
        )[0]

    def part_tokens(values, with_features):
        outs = [((local_len, features), low)] * images
        if with_features:
            outs += [((tokens, part), low)] * seq
        return local_call(
            functools.partial(tokens_out_kernel, images, seq),
            "part_tokens",
            info,
            [values],
            outs,
            [held_tokens, held_features],
        )

    def place_tokens(pieces):
        pieces = jnp.stack(pieces)
        return jnp.stack([pick(pieces, (j - depth) % images) for j in range(images)])

    def place_features(pieces):
        pieces = jnp.stack(pieces)
        rows = []
        for j in range(images):
            rows.append(
                jnp.concatenate(
                    [pick(pieces, (c * images + j - depth) % seq) for c in range(2)], axis=0
                )
            )
        return jnp.stack(rows)


    small = jnp.concatenate(
        [early_weight, later_weight, hidden_weight.reshape(-1, columns)], axis=0
    )
    small_count = small.shape[0]
    small_lanes = 64
    skip_width, reduce_width = skip_weight.shape[0], reduce_weight.shape[0]
    attend_count = attend_weight.shape[1] // columns
    expand_count = expand_weight.shape[1] // columns
    packed = list(local_call(
        functools.partial(pack_kernel, None, small_count),
        "pack",
        info,
        [skip_weight, attend_weight, output_weight, expand_weight, reduce_weight, small],
        [
            ((columns, skip_width + small_lanes), low),
            ((columns, (attend_count + 1) * depth_rows), low),
            ((columns, expand_count * depth_rows), low),
            ((columns, reduce_width), low),
        ],
    ))

    def send_depth(shard):
        return [shift(shard, r) for r in range(1, seq)]

    def join(shard, arrived, plan, outs):
        return local_call(
            functools.partial(join_kernel, plan, seq),
            "join",
            info,
            [shard] + arrived,
            [(shape, low) for shape in outs],
            [pltpu.VMEM((seq,) + shard.shape, low)],
        )

    def plan_skip(s):
        half = 2 * s // seq
        yield None, 0, skip_width, half, 0, (s - half * seq // 2) * skip_width
        if s == 0:
            yield None, skip_width, small_lanes, 1, 0, features

    def plan_reduce(s):
        half = 2 * s // seq
        yield None, 0, reduce_width, half, 0, (s - half * seq // 2) * reduce_width

    def plan_rows(count):
        def plan(s):
            for a in range(count):
                half = 2 * a // count
                row = (a - half * count // 2) * columns
                yield None, a * depth_rows, depth_rows, half, row, s * depth_rows

        return plan

    orders = (outer_bits, outer_bits[::-1])

    def exchange(halves, step):
        return [swap(x, orders[i][step]) for i, x in enumerate(halves)]

    def settle(halves, others, step):
        results = []
        for i, (mine, theirs) in enumerate(zip(halves, others)):
            bit = orders[i][step]
            inner = 2 ** sum(1 for b in orders[i][:step] if b < bit)
            total, rows, lanes = mine.shape
            shape = (total // inner, inner * rows, lanes)
            merged_half = merge(
                [mine.reshape(shape)],
                [theirs.reshape(shape)],
                info[2 + bit],
                ((0, 0, shape[1], 0, lanes, 0, 0, 0),),
                ((shape[1], lanes),),
            )[0]
            results.append(merged_half.reshape(2 * total, rows, lanes))
        return results

    def swap_core(halves):
        return [swap(x, 0) for x in halves]

    def complete(halves, others, plan, outs):
        return merge(list(halves), list(others), info[2], plan, outs)

    wave = len(outer_bits)


    half_rows = expand_count // 2 * columns
    mask_side = swap(key_keep, 0)
    arrived = send_depth(packed[0])
    arrived, packed[1] = tie((arrived, packed[1]))

    first = join(
        packed[0], arrived, plan_skip, [(columns, features), (columns, features + LANES)]
    )
    first = [x[None] for x in first]
    arrived = send_depth(packed[1])
    for step in range(wave):
        first = settle(first, exchange(first, step), step)
    arrived, first, packed[2] = tie((arrived, first, packed[2]))

    first_side = swap_core(first)
    second = join(
        packed[1], arrived, plan_rows(attend_count + 1), [(half_rows, features)] * 2
    )
    second = [x[None] for x in second]
    arrived = send_depth(packed[2])
    for step in range(wave):
        second = settle(second, exchange(second, step), step)
    slices = (token_slices(block_input), feature_slices(skip_input))
    arrived, first_side, second, slices = tie((arrived, first_side, second, slices))

    second_side = swap_core(second)
    third = join(packed[2], arrived, plan_rows(expand_count), [(half_rows, features)] * 2)
    third = [x[None] for x in third]
    input_pieces = send_tokens(slices[0])
    skip_pieces = send_features(slices[1])
    skip_full, small_full = complete(
        first,
        first_side,
        (
            (0, 0, columns, 0, features, 0, 0, 0),
            (1, 0, columns, 0, features, 0, 0, features),
            (1, 0, columns, features, features + LANES, 1, 0, 0),
        ),
        ((columns, 2 * features), (columns, LANES)),
    )
    skip_full = skip_full.reshape(features, 2 * features)
    small_rows = small_full.reshape(dp, columns, LANES)[:, :, :small_count].astype(jnp.float32)
    early_row = small_rows[:, :, :2].reshape(features, 2).T
    later_row = small_rows[:, :, 2:7].reshape(features, 5).T
    hidden_row = small_rows[:, :, 7:].transpose(0, 2, 1).reshape(hidden_width)
    for step in range(wave):
        third = settle(third, exchange(third, step), step)
    input_pieces, skip_pieces, third, second_side, packed[3], skip_full = tie(
        (input_pieces, skip_pieces, third, second_side, packed[3], skip_full)
    )

    line_keep = jnp.stack([key_keep, mask_side])
    line_keep = jnp.concatenate([pick(line_keep, core), pick(line_keep, 1 - core)], axis=0)
    image_keep = pick(line_keep, depth).reshape(2, tokens)
    gap = round_up(tokens, 16)
    pads = jnp.zeros((gap - tokens,), jnp.int32)
    mask = jnp.concatenate([pick(image_keep, core), pads, pick(image_keep, 1 - core), pads])

    arrived = send_depth(packed[3])
    third_side = swap_core(third)
    split_row = attend_count * columns - half_rows
    attend_full, output_full = complete(
        second,
        second_side,
        (
            (0, 0, half_rows, 0, features, 0, 0, 0),
            (1, 0, split_row, 0, features, 0, half_rows, 0),
            (1, split_row, half_rows, 0, features, 1, 0, 0),
        ),
        ((attend_count * columns, features), (columns, features)),
    )
    attend_full = attend_full.reshape(3 * features, features)
    output_full = output_full.reshape(features, features)
    inputs = join_tokens(input_pieces, skip_pieces)
    merged = matmul(inputs, skip_full, 1, 1) + early_row[1]
    normed_one, norm_one_back = jax.vjp(layer_norm, merged, later_row[0], early_row[0])
    normed_one_low = normed_one.astype(low)
    project = matmul(normed_one_low, attend_full, 1, 1).astype(low)
    key_values = project[:, features:]
    arrived, project, key_values, third_side = tie((arrived, project, key_values, third_side))

    sibling = swap(key_values, 0)
    fourth = join(
        packed[3], arrived, plan_reduce, [(columns, hidden_width // 2)] * 2
    )
    fourth = [x[None] for x in fourth]
    for step in range(wave - 1):
        fourth = settle(fourth, exchange(fourth, step), step)
    expand_full = complete(
        third,
        third_side,
        (
            (0, 0, half_rows, 0, features, 0, 0, 0),
            (1, 0, half_rows, 0, features, 0, half_rows, 0),
        ),
        ((2 * half_rows, features),),
    )[0].reshape(hidden_width, features)
    grad_slices = token_slices(output_grad)
    fourth, sibling, grad_slices, expand_full = tie((fourth, sibling, grad_slices, expand_full))

    grad_pieces = send_tokens(grad_slices)
    others = exchange(fourth, wave - 1)
    attended_low = attend_forward(project, sibling, mask[None, :])
    attended_low, others, grad_pieces = tie((attended_low, others, grad_pieces))

    fourth = settle(fourth, others, wave - 1)
    fourth_side = swap_core(fourth)
    middle = merged + matmul(attended_low, output_full, 1, 1) + later_row[3]
    normed_two, norm_two_back = jax.vjp(layer_norm, middle, later_row[1], later_row[2])
    normed_two_low = normed_two.astype(low)
    hidden_pre = matmul(normed_two_low, expand_full, 1, 1) + hidden_row
    activated, gelu_back = jax.vjp(gelu_exact, hidden_pre)
    activated_low = activated.astype(low)
    grad_out = join_tokens(grad_pieces)
    fourth_side, activated_low, grad_out = tie((fourth_side, activated_low, grad_out))


    core_bit = info[2]

    def places(step):
        spots = []
        for i in range(2):
            order = orders[i][::-1]
            left = sorted(b for b in outer_bits if b not in order[:step])
            spots.append((left.index(order[step]), 2 + order[step]))
        return tuple(spots)

    def view(gradient):
        return gradient.reshape(dp // 2, 2, -1, gradient.shape[-1])

    def send_parts(halves, step):
        return [swap(halves[2 * i + 1], orders[i][::-1][step]) for i in range(2)]

    def fold_next(halves, arrived, step):
        operands = [halves[0], arrived[0], halves[2], arrived[1]]
        outs = []
        for half in (halves[0], halves[2]):
            outs += [((half.shape[0] // 2,) + half.shape[1:], low)] * 2
        return local_call(
            functools.partial(fold_next_kernel, places(step)), "fold_next", info, operands, outs
        )

    def split(halves, arrived, plan, lanes):
        operands = [halves[0], arrived[0], halves[2], arrived[1]]
        return local_call(
            functools.partial(split_kernel, plan, seq, 2),
            "split",
            info,
            operands,
            [((columns, lanes), low)] * seq,
            [pltpu.VMEM((seq, columns, lanes), low)],
        )

    def send_chunks(chunks):
        return [chunks[0]] + [shift(chunks[r], r) for r in range(1, seq)]

    def halves_of_rows(rows, lanes):
        return ((0, rows // 2, 0, lanes), (rows // 2, rows, 0, lanes))

    def chunks_of_rows(count):
        plan = [[], []]
        for a in range(count):
            half = 2 * a // count
            row = (a - half * count // 2) * columns
            for s in range(seq):
                plan[half].append(
                    (s, row, columns, s * depth_rows, depth_rows, a * depth_rows)
                )
        return plan

    def chunks_of_lanes(width):
        plan = [[], []]
        for s in range(seq):
            half = 2 * s // seq
            plan[half].append((s, 0, columns, (s - half * seq // 2) * width, width, 0))
        return plan

    def adam(pieces, parts, states, shapes):
        operands = list(pieces)
        outs = []
        for state, shape in zip(states, shapes):
            operands += list(state)
            outs += [(shape, jnp.float32)] * 3 + [(shape, low)]
        return local_call(
            functools.partial(adam_kernel, seq, parts), "adam", info, operands, outs
        )


    grad_out_full = grad_out.astype(jnp.float32)
    reduce_grad = view(matmul(grad_out, activated_low, 0, 0).astype(low))
    reduce_send = carve([reduce_grad], core_bit)
    reduce_full = complete(
        fourth,
        fourth_side,
        (
            (0, 0, columns, 0, hidden_width // 2, 0, 0, 0),
            (1, 0, columns, 0, hidden_width // 2, 0, 0, hidden_width // 2),
        ),
        ((columns, hidden_width),),
    )[0].reshape(features, hidden_width)
    reduce_send, reduce_grad, reduce_full = tie((reduce_send, reduce_grad, reduce_full))

    from_core = swap(reduce_send, 0)
    block_output = (middle + matmul(activated_low, reduce_full, 1, 1) + later_row[4]).astype(low)
    output_pieces = part_tokens(block_output, False)
    from_core, output_pieces, grad_out_two = tie((from_core, output_pieces, grad_out))

    reduce_plan = ((0, columns, 0, hidden_width // 2), (0, columns, hidden_width // 2, hidden_width))
    reduce_halves = fold_first([reduce_grad], from_core, core_bit, info, reduce_plan, places(0))
    from_outer = send_parts(reduce_halves, 0)
    output_pieces = return_tokens(output_pieces)
    grad_act = matmul(grad_out_two, reduce_full, 1, 0)
    grad_pre_low = gelu_back(grad_act)[0].astype(low)
    hidden_grad = jnp.sum(grad_pre_low.astype(jnp.float32), axis=0)
    grad_normed_two = matmul(grad_pre_low, expand_full, 1, 0)
    from_outer, output_pieces, grad_pre_low, grad_normed_two = tie(
        (from_outer, output_pieces, grad_pre_low, grad_normed_two)
    )

    for step in range(1, wave):
        reduce_halves = fold_next(reduce_halves, from_outer, step)
        from_outer = send_parts(reduce_halves, step)
    expand_grad = view(matmul(grad_pre_low, normed_two_low, 0, 0).astype(low))
    expand_send = carve([expand_grad], core_bit)
    from_outer, expand_grad, expand_send = tie((from_outer, expand_grad, expand_send))

    from_core = swap(expand_send, 0)
    reduce_chunks = split(reduce_halves, from_outer, chunks_of_lanes(reduce_width), reduce_width)
    grad_middle_part, gain_two_grad, shift_two_grad = norm_two_back(grad_normed_two)
    grad_middle = grad_out_full + grad_middle_part
    grad_branch_low = grad_middle.astype(low)
    grad_attended = matmul(grad_branch_low, output_full, 1, 0).astype(low)
    from_core, reduce_chunks, grad_attended = tie((from_core, reduce_chunks, grad_attended))

    rows_plan = halves_of_rows(expand_count * columns, features)
    expand_halves = fold_first([expand_grad], from_core, core_bit, info, rows_plan, places(0))
    from_outer = send_parts(expand_halves, 0)
    reduce_pieces = send_chunks(reduce_chunks)
    own_grad, sibling_grad = attend_backward(project, sibling, mask[:, None], grad_attended)
    from_outer, reduce_pieces, own_grad, sibling_grad = tie(
        (from_outer, reduce_pieces, own_grad, sibling_grad)
    )

    returned = swap(sibling_grad, 0)
    for step in range(1, wave):
        expand_halves = fold_next(expand_halves, from_outer, step)
        from_outer = send_parts(expand_halves, step)
    output_weight_grad = view(matmul(grad_branch_low, attended_low, 0, 0).astype(low))
    project_grad = jnp.concatenate(
        [
            own_grad[:, :features],
            (
                own_grad[:, features:].astype(jnp.float32) + returned.astype(jnp.float32)
            ).astype(low),
        ],
        axis=1,
    )
    attend_grad = view(matmul(project_grad, normed_one_low, 0, 0).astype(low))
    attend_send = carve([attend_grad, output_weight_grad], core_bit)
    from_outer, attend_send, attend_grad, project_grad = tie(
        (from_outer, attend_send, attend_grad, project_grad)
    )

    from_core = swap(attend_send, 0)
    expand_chunks = split(
        expand_halves, from_outer, chunks_of_rows(expand_count), expand_count * depth_rows
    )
    grad_normed_one = matmul(project_grad, attend_full, 1, 0)
    grad_merged_part, gain_one_grad, shift_one_grad = norm_one_back(grad_normed_one)
    grad_merged_low = (grad_middle + grad_merged_part).astype(low)
    from_core, expand_chunks, grad_merged_low = tie((from_core, expand_chunks, grad_merged_low))

    attend_halves = fold_first(
        [attend_grad, output_weight_grad], from_core, core_bit, info, rows_plan, places(0)
    )
    from_outer = send_parts(attend_halves, 0)
    expand_pieces = send_chunks(expand_chunks)
    skip_grad_weight = matmul(grad_merged_low, inputs, 0, 0).astype(low)
    small_grad = jnp.concatenate(
        [
            jnp.stack(
                [
                    shift_one_grad,
                    jnp.sum(grad_merged_low.astype(jnp.float32), axis=0),
                    gain_one_grad,
                    gain_two_grad,
                    shift_two_grad,
                    jnp.sum(grad_branch_low.astype(jnp.float32), axis=0),
                    jnp.sum(grad_out_full, axis=0),
                ]
            ),
            hidden_grad.reshape(dp, -1, columns).transpose(1, 0, 2).reshape(-1, features),
        ],
        axis=0,
    ).astype(low)
    small_grad = jnp.pad(small_grad.T, ((0, 0), (0, LANES - small_count)))
    skip_grad_weight = view(jnp.concatenate([skip_grad_weight, small_grad], axis=1))
    skip_send = carve([skip_grad_weight], core_bit)
    grad_inputs = matmul(grad_merged_low, skip_full, 1, 0).astype(low)
    grad_pieces = part_tokens(grad_inputs, True)
    from_outer, expand_pieces, skip_send, grad_pieces = tie(
        (from_outer, expand_pieces, skip_send, grad_pieces)
    )

    from_core = swap(skip_send, 0)
    for step in range(1, wave):
        attend_halves = fold_next(attend_halves, from_outer, step)
        from_outer = send_parts(attend_halves, step)
    input_pieces = return_tokens(grad_pieces[:images])
    skip_pieces = return_features(grad_pieces[images:])
    reduce_results = adam(
        reduce_pieces,
        ((0, reduce_width, 1, step_rates[4]),),
        ((reduce_weight, reduce_first, reduce_second),),
        (reduce_weight.shape,),
    )
    from_core, from_outer, reduce_results = tie((from_core, from_outer, reduce_results))

    skip_plan = ((0, columns, 0, features), (0, columns, features, 2 * features + LANES))
    skip_halves = fold_first([skip_grad_weight], from_core, core_bit, info, skip_plan, places(0))
    from_skip = send_parts(skip_halves, 0)
    attend_chunks = split(
        attend_halves,
        from_outer,
        chunks_of_rows(attend_count + 1),
        (attend_count + 1) * depth_rows,
    )
    attend_pieces = send_chunks(attend_chunks)
    expand_results = adam(
        expand_pieces,
        ((0, depth_rows, expand_count, step_rates[3]),),
        ((expand_weight, expand_first, expand_second),),
        (expand_weight.shape,),
    )
    from_skip, input_pieces, skip_pieces, expand_results = tie(
        (from_skip, input_pieces, skip_pieces, expand_results)
    )

    for step in range(1, wave):
        skip_halves = fold_next(skip_halves, from_skip, step)
        from_skip = send_parts(skip_halves, step)
    input_grad = place_tokens(input_pieces)
    skip_grad = place_features(skip_pieces)
    from_skip, attend_pieces = tie((from_skip, attend_pieces))

    skip_chunk_plan = chunks_of_lanes(skip_width)
    for s in range(seq):
        skip_chunk_plan[1].append((s, 0, columns, features, small_lanes, skip_width))
    skip_pieces = send_chunks(
        split(skip_halves, from_skip, skip_chunk_plan, skip_width + small_lanes)
    )
    attend_results = adam(
        attend_pieces,
        (
            (0, depth_rows, attend_count, step_rates[1]),
            (attend_count * depth_rows, depth_rows, 1, step_rates[2]),
        ),
        (
            (attend_weight, attend_first, attend_second),
            (output_weight, output_first, output_second),
        ),
        (attend_weight.shape, output_weight.shape),
    )
    block_output = place_tokens(output_pieces)
    skip_pieces, attend_results = tie((skip_pieces, attend_results))

    stacked = [
        jnp.concatenate([a, b, c.reshape(-1, columns)], axis=0)
        for a, b, c in (
            (early_weight, later_weight, hidden_weight),
            (early_first, later_first, hidden_first),
            (early_second, later_second, hidden_second),
        )
    ]
    skip_results = adam(
        skip_pieces,
        ((0, skip_width, 1, step_rates[0]),),
        ((skip_weight, skip_first, skip_second),),
        (skip_weight.shape,),
    )
    small_total = skip_pieces[0][:, skip_width:].astype(jnp.float32)
    for piece in skip_pieces[1:]:
        small_total = small_total + piece[:, skip_width:].astype(jnp.float32)
    small_total = small_total.T[:small_count]
    rate_rows = jnp.repeat(
        jnp.array(step_rates[5:8], jnp.float32),
        jnp.array([2, 5, small_count - 7]),
        total_repeat_length=small_count,
    )[:, None]
    small_results = adamw_update(stacked[0], stacked[1], stacked[2], small_total, rate_rows)

    results = [block_output, input_grad, skip_grad]
    results += list(skip_results)
    results += list(attend_results)
    results += list(expand_results)
    results += list(reduce_results)
    results += [x[:2] for x in small_results]
    results += [x[2:7] for x in small_results]
    results += [x[7:].reshape(1, -1) for x in small_results]
    return tuple(results)


def solution(mesh):
    sizes = (mesh.shape["dp"], mesh.shape["seq"])
    matrix, row = P("seq", "dp"), P(None, "dp")
    token, feature = P("dp", "seq", None), P("dp", None, "seq")
    return jax.shard_map(
        functools.partial(shards, sizes),
        mesh=mesh,
        in_specs=(token, feature, P("dp", None), token) + (matrix,) * 15 + (row,) * 9,
        out_specs=(token, token, feature) + (matrix,) * 20 + (row,) * 12,
        check_vma=False,
    )
```
